32 devices in a mesh: dp: 4 (over x, core), fsdp: 8 (over z, y).
Axes of the slice: x: 2, y: 2, z: 4, core: 2. Of those that a mesh axis runs over, the one named last changes fastest.
Arguments:
- hidden: bfloat16 [32, 256, 4096], P(('dp', 'fsdp')), may hold values from -40 to 40
- lengths: int32 [32], P(('dp', 'fsdp')), may hold values from 64 to 256
- list_ids: int32 [32], P('dp'), may hold values from 0 to 255, as said below
- list_owner: int32 [256], replicated, may hold values from 0 to 3, as said below
- attn_gain: float32 [4096], replicated, may hold values from 0.25 to 1.75
- final_gain: float32 [4096], replicated, may hold values from 0.25 to 1.75
- w_query: bfloat16 [4096, 2048], P('fsdp'), may hold values from -24 to 24
- w_key: bfloat16 [4096, 512], P('fsdp'), may hold values from -1 to 1
- w_value: bfloat16 [4096, 512], P('fsdp'), may hold values from -0.09375 to 0.09375
- w_out: bfloat16 [2048, 4096], P('fsdp'), may hold values from -0.125 to 0.125
Outputs:
- inbox: bfloat16 [4, 4, 4, 4096], P('dp', None, None, 'fsdp')
The draws below stay inside these ranges and needn't reach their ends.
Inputs may be any that keep to these rules, and one draw needn't show every extreme that they name: Positions from lengths[p] on are padding. `list_ids`: in each aligned block of 8 passages (those of one index of dp), at most 4 passages name lists of one owner, and in every block some owner is named by exactly 4 passages. `list_owner`: every owner holds exactly 64 lists.
All inputs are finite; a program needn't handle non-finite values.
Results may differ from the reference program's by a relative error of at most 0.0029.
The reference program's roundings to bfloat16 on the way (of `normed`, `key_rows`, `queries`, `weights`, `context` and `embedded`) count: a program that leaves them out, or rounds other values in their place, can miss the bound.
Values may be sent and summed in bfloat16 or wider, within the bound.
A program may use at most 64 MiB of HBM per device.

```python
import math
import jax
import jax.numpy as jnp
from jax import lax

D = 4096
HEADS = 16
KV_HEADS = 4
HEAD = 128
LEN = 256
PASSAGES = 32
LISTS = 256
CAP = 4
N_DP = 4


def owner_order(key):
    return jax.random.permutation(jax.random.fold_in(key, 7), LISTS)


def draw_list_owner(key, part):
    return (owner_order(key) % N_DP).astype(jnp.int32)


def draw_list_ids(key, part):
    inverse = jnp.argsort(owner_order(key))
    block_size = PASSAGES // N_DP
    slot_count = N_DP * CAP
    slot_owner = jnp.arange(slot_count) // CAP
    crowded = jax.random.randint(jax.random.fold_in(key, 8), (), 0, N_DP)

    def one_block(index):
        block_key = jax.random.fold_in(jax.random.fold_in(key, 9), index)
        noise = jax.random.randint(jax.random.fold_in(block_key, 1), (slot_count,), 0, 1 << 20)
        ranking = jnp.where(slot_owner == crowded, jnp.arange(slot_count), (noise + 1) * slot_count + jnp.arange(slot_count))
        chosen = slot_owner[jnp.argsort(ranking)[:block_size]]
        mixing = jax.random.randint(jax.random.fold_in(block_key, 2), (block_size,), 0, 1 << 20) * block_size + jnp.arange(block_size)
        owners = chosen[jnp.argsort(mixing)]
        choice_in_owner = jax.random.randint(jax.random.fold_in(block_key, 3), (block_size,), 0, LISTS // N_DP)
        return inverse[owners + N_DP * choice_in_owner]
    return jax.vmap(one_block)(jnp.arange(N_DP)).reshape(PASSAGES).astype(jnp.int32)


def key_base(key):
    drawn = jax.random.normal(jax.random.fold_in(key, 21), (D, KV_HEADS * HEAD), jnp.float32)
    return jnp.clip(drawn, -6.0, 6.0) / math.sqrt(D)


def draw_w_key(key, part):
    return key_base(key).astype(jnp.bfloat16)


def draw_w_query(key, part):
    drawn = jax.random.normal(jax.random.fold_in(key, 22), (D, HEADS * HEAD), jnp.float32)
    own_part = jnp.clip(drawn, -6.0, 6.0) / math.sqrt(D)
    return own_part.astype(jnp.bfloat16)


def draw_hidden(key, part):
    drawn = jax.random.normal(jax.random.fold_in(key, 31), (PASSAGES, LEN, D), jnp.float32)
    return jnp.clip(drawn, -6.0, 6.0).astype(jnp.bfloat16)


def set_ends(values, rng, low, largest):
    extent = values.shape
    index_at = [jax.random.randint(jax.random.fold_in(rng, axis), (), 0, extent[axis]) for axis in range(len(extent))]
    values = values.at[tuple(index_at)].set(low)
    longest = extent.index(max(extent))
    index_at[longest] = (index_at[longest] + 1) % extent[longest]
    return values.at[tuple(index_at)].set(largest)


def levels(own_key, extent, cuts, low, largest):
    factor_of, own = 1.0, jax.random.fold_in(own_key, 6)
    for dim, blocks in cuts:
        steps = jnp.exp(jax.random.uniform(jax.random.fold_in(own, dim), (blocks,), jnp.float32, low / len(cuts), largest / len(cuts)))
        factor_of = factor_of * jnp.repeat(steps, extent[dim] // blocks).reshape([-1 if axis == dim else 1 for axis in range(len(extent))])
    return factor_of


def centred(key, extent, scale, limit, split=(), kind=jnp.bfloat16):
    result = jax.random.normal(key, extent, jnp.float32) * scale
    if len(split) > 0:
        result = levels(key, extent, split, -0.22, 0.18) * result
    return jnp.clip(result, min=-limit, max=limit).astype(kind)


def setup_inputs(seed: int = 0) -> dict:
    seeds = jax.random.split(jax.random.key(seed), 11)
    return {
        "hidden": draw_hidden(jax.random.fold_in(seeds[10], 71), 0),
        "lengths": set_ends(jax.random.randint(seeds[1], (PASSAGES,), LEN // 4, LEN + 1), jax.random.fold_in(seeds[1], 1), LEN // 4, LEN).astype(jnp.int32),
        "list_ids": draw_list_ids(jax.random.fold_in(seeds[10], 71), 0),
        "list_owner": draw_list_owner(jax.random.fold_in(seeds[10], 71), 0),
        "attn_gain": jnp.clip(1.0 + 0.15 * jax.random.normal(seeds[4], (D,), jnp.float32), 0.25, 1.75),
        "final_gain": jnp.clip(1.0 + 0.15 * jax.random.normal(seeds[5], (D,), jnp.float32), 0.25, 1.75),
        "w_query": draw_w_query(jax.random.fold_in(seeds[10], 71), 0),
        "w_key": draw_w_key(jax.random.fold_in(seeds[10], 71), 0),
        "w_value": centred(seeds[8], (D, KV_HEADS * HEAD), D ** -0.5, 0.09375, ((0, 8),)),
        "w_out": centred(seeds[9], (HEADS * HEAD, D), (HEADS * HEAD) ** -0.5, 0.125, ((0, 8),)),
    }


def rope_tables(positions, head_width):
    halfway = head_width // 2
    frequency = 10000.0 ** (-jnp.arange(halfway, dtype=jnp.float32) * 2.0 / head_width)
    angles = positions.astype(jnp.float32)[..., None] * frequency
    return (jnp.cos(angles), jnp.sin(angles))

def rotate(vectors, cosine_table, sine_table):
    halfway = vectors.shape[-1] // 2
    first_half = vectors[..., :halfway]
    second_half = vectors[..., halfway:]
    return jnp.concatenate([first_half * cosine_table - second_half * sine_table, second_half * cosine_table + first_half * sine_table], axis=-1)

def reference(hidden, lengths, list_ids, list_owner, attn_gain, final_gain, w_query, w_key, w_value, w_out):
    cosine_table, sine_table = rope_tables(jnp.arange(LEN), HEAD)

    def embed_one(inputs):
        passage, length = inputs
        floats = passage.astype(jnp.float32)
        normed = (floats * lax.rsqrt(lax.optimization_barrier(jnp.mean(floats * floats, axis=-1, keepdims=True)) + 1e-05) * attn_gain).astype(jnp.bfloat16)
        key_sum = jnp.dot(normed, w_key, preferred_element_type=jnp.float32).reshape(LEN, KV_HEADS, HEAD)
        key_rows = rotate(key_sum, cosine_table[:, None, :], sine_table[:, None, :]).astype(jnp.bfloat16)
        value_rows = jnp.dot(normed, w_value, preferred_element_type=jnp.float32).reshape(LEN, KV_HEADS, HEAD)
        last_position = length - 1
        last_normed = lax.dynamic_index_in_dim(normed, last_position, 0, keepdims=False)
        last_input = lax.dynamic_index_in_dim(passage, last_position, 0, keepdims=False).astype(jnp.float32)
        query_sum = jnp.dot(last_normed, w_query, preferred_element_type=jnp.float32).reshape(HEADS, HEAD)
        query_cos, query_sin = rope_tables(last_position[None], HEAD)
        queries = (rotate(query_sum, query_cos, query_sin) * (1.0 / math.sqrt(HEAD))).astype(jnp.bfloat16)
        grouped = queries.reshape(KV_HEADS, HEADS // KV_HEADS, HEAD).astype(jnp.float32)
        scores = jnp.einsum('kgd,tkd->kgt', grouped, key_rows.astype(jnp.float32))
        visible = jnp.arange(LEN)[None, None, :] < length
        scores = jnp.where(visible, scores, -jnp.inf)
        powers = jnp.exp(scores - lax.optimization_barrier(jnp.max(scores, axis=-1, keepdims=True)))
        weights = (powers / lax.optimization_barrier(jnp.sum(powers, axis=-1, keepdims=True))).astype(jnp.bfloat16)
        context = jnp.einsum('kgt,tkd->kgd', weights.astype(jnp.float32), value_rows, precision=lax.Precision.HIGHEST)
        context = context.reshape(HEADS * HEAD).astype(jnp.bfloat16)
        residual = last_input + jnp.dot(context, w_out, preferred_element_type=jnp.float32)
        scaled = residual * final_gain
        return (scaled * lax.rsqrt(jnp.mean(scaled * scaled) + 1e-06)).astype(jnp.bfloat16)
    embedded = lax.map(embed_one, (hidden, lengths))
    block_size = PASSAGES // N_DP
    owners = list_owner[list_ids].reshape(N_DP, block_size)
    owner_marks = (owners[:, :, None] == jnp.arange(N_DP)[None, None, :]).astype(jnp.int32)
    slot_rank = lax.optimization_barrier(jnp.sum((jnp.cumsum(owner_marks, axis=1) - owner_marks) * owner_marks, axis=2))
    select = ((owners[:, None, None, :] == jnp.arange(N_DP)[None, :, None, None]) & (slot_rank[:, None, None, :] == jnp.arange(CAP)[None, None, :, None])).astype(jnp.float32)
    grouped_rows = embedded.reshape(N_DP, block_size, D).astype(jnp.float32)
    inbox = jnp.einsum('josr,jrd->ojsd', select, grouped_rows, precision=lax.Precision.HIGHEST)
    return inbox.astype(jnp.bfloat16)
```

```python
import functools
import math

import jax
import jax.numpy as jnp
import numpy as np
from jax import lax
from jax.experimental import pallas as pl
from jax.experimental.pallas import tpu as pltpu
from jax.sharding import PartitionSpec as P

HEADS = 16
KV_HEADS = 4
HEAD = 128
GROUP = HEADS // KV_HEADS
MESH = pl.DeviceIdType.MESH
F32 = jnp.float32
BF16 = jnp.bfloat16


def rope_tables(seq_len):
    half = HEAD // 2
    exponent = -np.arange(half, dtype=np.float32) * np.float32(2.0) / np.float32(HEAD)
    frequency = (np.float64(10000.0) ** exponent.astype(np.float64)).astype(np.float32)
    angles = (np.arange(seq_len, dtype=np.float32)[:, None] * frequency).astype(np.float64)
    cosine, sine = np.cos(angles), np.sin(angles)
    return (
        np.concatenate([cosine, cosine], axis=1).astype(np.float32),
        np.concatenate([-sine, sine], axis=1).astype(np.float32),
    )


def kernel(
    n_dp, n, chunks,
    lengths, list_ids,
    owners_hbm, hidden_hbm, again_hbm, fgain_hbm, cos_hbm, sin_hbm, wq_hbm, wk_hbm, wv_hbm, wo_hbm,
    out_ref,
    hid, normed, again, fgain, cos_t, sin_t, wq, wk, wv, wo,
    owners, acc, last_in, gain2,
    x_send, x_recv, q_send, q_recv, u_send, u_recv, mixed, c_send, c_recv, o_send, o_recv,
    e_send, e_recv,
    load_sem, a2a_send, a2a_recv,
    zu_s, zd_s, y_s, x_s, dz_s, dy_s, dx_s, z_r, y_r, x_r, dz_r, dy_r, dx_r,
):
    dp = lax.axis_index("dp")
    f = lax.axis_index("fsdp")
    seq_len, width = hid.shape
    slab = width // n
    depth = n // 2
    total = n_dp * n
    cap = out_ref.shape[2]
    a, b = f // 2, f % 2
    core, x_bit = dp % 2, (dp // 2) % 2
    partner = dp + 1 - 2 * core
    x_peer = dp + 2 - 4 * x_bit

    sources = (wk_hbm, hidden_hbm.at[0], again_hbm, wq_hbm, cos_hbm, sin_hbm, wv_hbm, wo_hbm, fgain_hbm,
               owners_hbm)
    targets = (wk.at[f], hid, again, wq, cos_t, sin_t, wv, wo, fgain, owners)
    loads = [
        pltpu.make_async_copy(s, t, load_sem.at[i])
        for i, (s, t) in enumerate(zip(sources, targets))
    ]
    for load in loads:
        load.start()

    me = dp * n + f
    barrier = pltpu.get_barrier_semaphore()

    def greet(t, carry):
        other = lax.rem(me + t, total)
        pl.semaphore_signal(
            barrier, inc=1, device_id=(other // n, other % n), device_id_type=MESH
        )
        return carry

    lax.fori_loop(1, total, greet, 0)
    pl.semaphore_wait(barrier, total - 1)

    step = slab // chunks

    def piece(pa, pb, offset, rows, send_sem, recv_sem, device):
        part = wk.at[pa * 2 + pb, pl.ds(pl.multiple_of(offset, rows), rows), :]
        return pltpu.make_async_remote_copy(
            src_ref=part, dst_ref=part, send_sem=send_sem, recv_sem=recv_sem,
            device_id=device, device_id_type=MESH,
        )

    def half_at(k, c):
        return k * step + c * (step // 2)

    def quarter_at(k, c, x):
        return half_at(k, c) + x * (step // 4)

    half, quarter = step // 2, step // 4

    def up(pa, k):
        return piece(pa, b, half_at(k, core), half, zu_s.at[pa, k], z_r.at[pa, k], (dp, lax.rem(f + 2, n)))

    def down(pa, k):
        return piece(pa, b, half_at(k, core), half, zd_s.at[pa, k], z_r.at[pa, k], (dp, lax.rem(f + n - 2, n)))

    def cross_y(pa, pb, k):
        return piece(pa, pb, quarter_at(k, core, x_bit), quarter, y_s.at[pa, k], y_r.at[pa, k], (dp, 2 * a + 1 - b))

    def cross_x(pa, k, x):
        return piece(pa, 1 - b, quarter_at(k, core, x), quarter, x_s.at[pa, k], x_r.at[pa, k], (x_peer, f))

    def core_z(pa, k, c):
        return piece(pa, b, half_at(k, c), half, dz_s.at[pa, k], dz_r.at[pa, k], (partner, f))

    def core_y(pa, k, c):
        return piece(pa, 1 - b, quarter_at(k, c, x_bit), quarter, dy_s.at[pa, k], dy_r.at[pa, k], (partner, f))

    def core_x(pa, k, c):
        return piece(pa, 1 - b, quarter_at(k, c, 1 - x_bit), quarter, dx_s.at[pa, k], dx_r.at[pa, k], (partner, f))

    loads[0].wait()
    for k in range(chunks):
        @pl.when(a < depth - 1)
        def _():
            up(a, k).start()

        @pl.when(a > 0)
        def _():
            down(a, k).start()

        cross_y(a, b, k).start()

    def exchange(slot, send, recv):
        def one(t, carry):
            g = lax.rem(f + t, n)
            pltpu.make_async_remote_copy(
                src_ref=send.at[g], dst_ref=recv.at[f], send_sem=a2a_send.at[slot],
                recv_sem=a2a_recv.at[slot], device_id=(dp, g), device_id_type=MESH,
            ).start()
            return carry

        lax.fori_loop(1, n, one, 0)
        recv[f] = send[f]

    def arrived(slot, recv, count):
        blocks = recv.at[pl.ds(0, count)]
        pltpu.make_async_copy(blocks, blocks, a2a_recv.at[slot]).wait()

    def sent(slot, recv, count):
        blocks = recv.at[pl.ds(0, count)]
        pltpu.make_async_copy(blocks, blocks, a2a_send.at[slot]).wait()

    loads[1].wait()
    loads[2].wait()
    last = lengths[0] - 1
    picks = lax.broadcasted_iota(jnp.int32, (16, seq_len), 1) == last
    picks = jnp.where(picks, 1.0, 0.0).astype(BF16)
    row = jnp.concatenate(
        [
            jnp.dot(picks, hid[:, g * slab:(g + 1) * slab], preferred_element_type=F32)[:1]
            for g in range(n)
        ],
        axis=1,
    )
    scale = lax.rsqrt(jnp.mean(row * row, axis=-1, keepdims=True) + 1e-05)
    row_normed = (row * scale * again[...]).astype(BF16).astype(F32)
    for g in range(n):
        x_send[g] = row_normed[:, g * slab:(g + 1) * slab]
        last_in[g:g + 1, :] = row[:, g * slab:(g + 1) * slab]
    exchange(0, x_send, x_recv)

    block = 16

    def normalise(i, carry):
        window = pl.ds(pl.multiple_of(i * block, block), block)
        x = hid[window, :].astype(F32)
        r = lax.rsqrt(jnp.mean(x * x, axis=-1, keepdims=True) + 1e-05)
        normed[window, :] = (x * r * again[...]).astype(BF16)
        return carry

    lax.fori_loop(0, seq_len // block, normalise, 0)

    loads[3].wait()
    arrived(0, x_recv, n - 1)
    x_all = jnp.concatenate([x_recv[i] for i in range(n)], axis=0).astype(BF16)
    for h in range(HEADS):
        q_send[:, h, :] = jnp.dot(
            x_all, wq[:, h * HEAD:(h + 1) * HEAD], preferred_element_type=F32
        )
    exchange(1, q_send, q_recv)

    acc[...] = jnp.zeros_like(acc)

    def accumulate(slab_index):
        columns = pl.ds(pl.multiple_of(slab_index * slab, slab), slab)
        acc[...] += jnp.dot(normed[:, columns], wk[slab_index], preferred_element_type=F32)

    accumulate(f)

    def around(e, body):
        for sign in (1, -1):
            pa = a + sign * e
            valid = (pa >= 0) & (pa < depth) & (e >= (0 if sign == 1 else 1))

            @pl.when(valid)
            def _():
                body(pa, sign)

    def gather_step(d, carry):
        def from_z(pa, sign):
            for k in range(chunks):
                up(pa, k).wait_recv()
                if sign == 1:
                    @pl.when(a > 0)
                    def _():
                        down(pa, k).start()
                else:
                    @pl.when(a < depth - 1)
                    def _():
                        up(pa, k).start()
                cross_y(pa, b, k).start()
                core_z(pa, k, core).start()

        def from_y(pa, sign):
            for k in range(chunks):
                cross_y(pa, 1 - b, k).wait_recv()
                cross_x(pa, k, x_bit).start()
                core_y(pa, k, core).start()

        def from_x(pa, sign):
            for k in range(chunks):
                cross_x(pa, k, 1 - x_bit).wait_recv()
                core_x(pa, k, core).start()

        def consume(pa, sign):
            @pl.when(pa != a)
            def _():
                for k in range(chunks):
                    core_z(pa, k, 1 - core).wait_recv()
                accumulate(pa * 2 + b)

            for k in range(chunks):
                core_y(pa, k, 1 - core).wait_recv()
                core_x(pa, k, 1 - core).wait_recv()
            accumulate(pa * 2 + 1 - b)

        @pl.when(d >= 1)
        def _():
            around(d, from_z)
            around(d - 1, from_y)
            around(d - 1, from_x)

        @pl.when(d >= 2)
        def _():
            around(d - 2, consume)

        return carry

    lax.fori_loop(1, depth + 2, gather_step, 0)

    for load in loads[4:]:
        load.wait()
    arrived(1, q_recv, n - 1)
    queries = jnp.sum(q_recv[...], axis=0)
    at_last = lax.broadcasted_iota(jnp.int32, cos_t.shape, 0) == last
    q_cos = jnp.sum(jnp.where(at_last, cos_t[...], 0.0), axis=0, keepdims=True)
    q_sin = jnp.sum(jnp.where(at_last, sin_t[...], 0.0), axis=0, keepdims=True)
    queries = queries * q_cos + pltpu.roll(queries, HEAD // 2, 1) * q_sin
    queries = (queries * (1.0 / math.sqrt(HEAD))).astype(BF16)

    scores = jnp.zeros((HEADS, seq_len), F32)
    head_of = lax.broadcasted_iota(jnp.int32, scores.shape, 0) // GROUP
    for kv in range(KV_HEADS):
        keys = acc[:, kv * HEAD:(kv + 1) * HEAD]
        keys = (keys * cos_t[...] + pltpu.roll(keys, HEAD // 2, 1) * sin_t[...]).astype(BF16)
        part = lax.dot_general(queries, keys, (((1,), (1,)), ((), ())), preferred_element_type=F32)
        scores = jnp.where(head_of == kv, part, scores)
    visible = lax.broadcasted_iota(jnp.int32, scores.shape, 1) < lengths[0]
    scores = jnp.where(visible, scores, -jnp.inf)
    powers = jnp.exp(scores - jnp.max(scores, axis=-1, keepdims=True))
    weights = (powers / jnp.sum(powers, axis=-1, keepdims=True)).astype(BF16)

    for g in range(n):
        u_send[g] = jnp.dot(weights, normed[:, g * slab:(g + 1) * slab], preferred_element_type=F32)
    exchange(2, u_send, u_recv)
    arrived(2, u_recv, n - 1)
    sums = u_recv[...].reshape(n * HEADS, slab)
    top = sums.astype(BF16)
    rest = sums - top.astype(F32)
    middle = rest.astype(BF16)
    low = (rest - middle.astype(F32)).astype(BF16)
    values = wv[...]
    product = (
        jnp.dot(low, values, preferred_element_type=F32)
        + jnp.dot(middle, values, preferred_element_type=F32)
    ) + jnp.dot(top, values, preferred_element_type=F32)
    for kv in range(KV_HEADS):
        mixed[kv] = product[:, kv * HEAD:(kv + 1) * HEAD]

    share = HEADS * HEAD // n
    for h in range(HEADS):
        kv = h // GROUP
        part = mixed[kv, pl.ds(h, n, stride=HEADS), :]
        if share >= HEAD:
            at = h * HEAD % share
            c_send[h * HEAD // share, :, at:at + HEAD] = part
        else:
            pieces = HEAD // share
            for i in range(pieces):
                c_send[h * pieces + i] = part[:, i * share:(i + 1) * share]
    exchange(3, c_send, c_recv)
    arrived(3, c_recv, n - 1)
    context = jnp.sum(c_recv[...], axis=0).astype(BF16)
    for g in range(n):
        o_send[:, g, :] = jnp.dot(
            context, wo[:, g * slab:(g + 1) * slab], preferred_element_type=F32
        )
        gain2[g:g + 1, :] = fgain[:, g * slab:(g + 1) * slab]
    exchange(4, o_send, o_recv)

    lists = lax.broadcasted_iota(jnp.int32, owners.shape, 1)

    def owner_of(r):
        held = jnp.where(lists == list_ids[r], owners[...], 0)
        return jnp.sum(held.astype(F32), axis=1, keepdims=True)

    owner = owner_of(f)

    def count(r, slot):
        same = jnp.where(owner_of(r) == owner, 1.0, 0.0)
        return slot + same * jnp.where(r < f, 1.0, 0.0)

    code = owner * cap + lax.fori_loop(0, n, count, jnp.zeros((1, 1), F32))

    arrived(4, o_recv, n - 1)
    scaled = (last_in[...] + jnp.sum(o_recv[...], axis=0)) * gain2[...]
    square = jnp.sum(jnp.sum(scaled * scaled, axis=1, keepdims=True), axis=0, keepdims=True)
    embedded = (scaled * lax.rsqrt(square / width + 1e-06)).astype(BF16).astype(F32)
    for g in range(n):
        e_send[g, :, :slab] = embedded[g:g + 1, :]
        e_send[g, :, slab:] = jnp.broadcast_to(code, (1, 128))

    def post(t, carry):
        other = lax.rem(me + t, total)
        g = other % n
        pltpu.make_async_remote_copy(
            src_ref=e_send.at[g], dst_ref=e_recv.at[me], send_sem=a2a_send.at[5],
            recv_sem=a2a_recv.at[5], device_id=(other // n, g), device_id_type=MESH,
        ).start()
        return carry

    lax.fori_loop(1, total, post, 0)
    e_recv[me] = e_send[f]
    arrived(5, e_recv, total - 1)

    first = (dp * cap).astype(F32)
    for j in range(n_dp):
        rows = jnp.concatenate([e_recv[j * n + i] for i in range(n)], axis=0)
        codes = rows[:, slab:slab + 1]
        for s in range(cap):
            kept = jnp.where(codes == first + s, rows[:, :slab], 0.0)
            out_ref[0, j, s:s + 1, :] = jnp.sum(kept, axis=0, keepdims=True).astype(BF16)

    for index, recv in ((0, x_recv), (1, q_recv), (2, u_recv), (3, c_recv), (4, o_recv)):
        sent(index, recv, n - 1)
    sent(5, e_recv, total - 1)

    def drain(pa, carry):
        for k in range(chunks):
            @pl.when((pa <= a) & (a < depth - 1))
            def _():
                up(pa, k).wait_send()

            @pl.when((pa >= a) & (a > 0))
            def _():
                down(pa, k).wait_send()

            @pl.when(pa != a)
            def _():
                core_z(pa, k, core).wait_send()

            cross_y(pa, b, k).wait_send()
            cross_x(pa, k, x_bit).wait_send()
            core_y(pa, k, core).wait_send()
            core_x(pa, k, core).wait_send()
        return carry

    lax.fori_loop(0, depth, drain, 0)


def local(
    n_dp, n,
    hidden, lengths, list_ids, list_owner, attn_gain, final_gain, w_query, w_key, w_value, w_out,
):
    _, seq_len, width = hidden.shape
    slab = width // n
    depth = n // 2
    chunks = 2 if n <= 8 else 1
    cap = max(2, 2 * n // n_dp)
    share = HEADS * HEAD // n
    cosine, sine = rope_tables(seq_len)
    pieces = pltpu.SemaphoreType.DMA((depth, chunks))
    any_spec = pl.BlockSpec(memory_space=pl.ANY)
    smem_spec = pl.BlockSpec(memory_space=pltpu.SMEM)
    vmem = pltpu.VMEM
    return pl.pallas_call(
        functools.partial(kernel, n_dp, n, chunks),
        out_shape=jax.ShapeDtypeStruct((1, n_dp, cap, slab), BF16),
        in_specs=[smem_spec] * 2 + [any_spec] * 10,
        out_specs=pl.BlockSpec(memory_space=pltpu.VMEM),
        scratch_shapes=[
            vmem((seq_len, width), BF16),
            vmem((seq_len, width), BF16),
            vmem((1, width), F32),
            vmem((1, width), F32),
            vmem((seq_len, HEAD), F32),
            vmem((seq_len, HEAD), F32),
            vmem(w_query.shape, BF16),
            vmem((n,) + w_key.shape, BF16),
            vmem(w_value.shape, BF16),
            vmem(w_out.shape, BF16),
            vmem((1, list_owner.shape[0]), jnp.int32),
            vmem((seq_len, KV_HEADS * HEAD), F32),
            vmem((n, slab), F32),
            vmem((n, slab), F32),
            vmem((n, 1, slab), F32),
            vmem((n, 1, slab), F32),
            vmem((n, HEADS, HEAD), F32),
            vmem((n, HEADS, HEAD), F32),
            vmem((n, HEADS, slab), F32),
            vmem((n, HEADS, slab), F32),
            vmem((KV_HEADS, n * HEADS, HEAD), F32),
            vmem((n, n, share), F32),
            vmem((n, n, share), F32),
            vmem((n, n, slab), F32),
            vmem((n, n, slab), F32),
            vmem((n, 1, slab + 128), F32),
            vmem((n_dp * n, 1, slab + 128), F32),
            pltpu.SemaphoreType.DMA((10,)),
            pltpu.SemaphoreType.DMA((6,)),
            pltpu.SemaphoreType.DMA((6,)),
        ] + [pieces] * 13,
        compiler_params=pltpu.CompilerParams(
            collective_id=0, has_side_effects=True, vmem_limit_bytes=67043328
        ),
    )(
        lengths, list_ids,
        list_owner.reshape(1, -1), hidden, attn_gain.reshape(1, width), final_gain.reshape(1, width),
        cosine, sine, w_query, w_key, w_value, w_out,
    )


def solution(mesh):
    in_specs = (
        P(("dp", "fsdp"), None, None),
        P(("dp", "fsdp")),
        P("dp"),
        P(),
        P(),
        P(),
        P("fsdp", None),
        P("fsdp", None),
        P("fsdp", None),
        P("fsdp", None),
    )
    out_specs = P("dp", None, None, "fsdp")
    body = functools.partial(local, mesh.shape["dp"], mesh.shape["fsdp"])
    return jax.shard_map(body, mesh=mesh, in_specs=in_specs, out_specs=out_specs, check_vma=False)
```

```python
import functools
import math

import jax
import jax.numpy as jnp
import numpy as np
from jax import lax
from jax.experimental import pallas as pl
from jax.experimental.pallas import tpu as pltpu
from jax.sharding import PartitionSpec as P

HEADS = 16
KV_HEADS = 4
HEAD = 128
GROUP = HEADS // KV_HEADS
MESH = pl.DeviceIdType.MESH
F32 = jnp.float32
BF16 = jnp.bfloat16


def rope_tables(seq_len):
    half = HEAD // 2
    exponent = -np.arange(half, dtype=np.float32) * np.float32(2.0) / np.float32(HEAD)
    frequency = (np.float64(10000.0) ** exponent.astype(np.float64)).astype(np.float32)
    angles = (np.arange(seq_len, dtype=np.float32)[:, None] * frequency).astype(np.float64)
    cosine, sine = np.cos(angles), np.sin(angles)
    return (
        np.concatenate([cosine, cosine], axis=1).astype(np.float32),
        np.concatenate([-sine, sine], axis=1).astype(np.float32),
    )


def kernel(
    n_dp, n, chunks,
    lengths, list_ids,
    owners_hbm, hidden_hbm, again_hbm, fgain_hbm, cos_hbm, sin_hbm, wq_hbm, wk_hbm, wv_hbm, wo_hbm,
    out_ref,
    hid, normed, again, fgain, cos_t, sin_t, wq, wk, wv, wo,
    owners, acc, last_in, gain2,
    x_send, x_recv, q_send, q_recv, u_send, u_recv, mixed, c_send, c_recv, o_send, o_recv,
    e_send, e_recv,
    load_sem, a2a_send, a2a_recv, round_sem,
    zu_s, zd_s, y_s, x_s, dz_s, dy_s, dx_s, z_r, y_r, x_r, dz_r, dy_r, dx_r,
):
    dp = lax.axis_index("dp")
    f = lax.axis_index("fsdp")
    seq_len, width = hid.shape
    slab = width // n
    depth = n // 2
    total = n_dp * n
    cap = out_ref.shape[2]
    a, b = f // 2, f % 2
    core, x_bit = dp % 2, (dp // 2) % 2
    partner = dp + 1 - 2 * core
    x_peer = dp + 2 - 4 * x_bit

    sources = (wk_hbm, hidden_hbm.at[0], again_hbm, wq_hbm, cos_hbm, sin_hbm, wv_hbm, wo_hbm, fgain_hbm,
               owners_hbm)
    targets = (wk.at[f], hid, again, wq, cos_t, sin_t, wv, wo, fgain, owners)
    loads = [
        pltpu.make_async_copy(s, t, load_sem.at[i])
        for i, (s, t) in enumerate(zip(sources, targets))
    ]
    for load in loads:
        load.start()

    me = dp * n + f

    def wrap(index, size):
        return jnp.where(index >= size, index - size, index)

    def each(low, high, body):
        if high <= 8:
            for t in range(low, high):
                body(t)
        else:
            lax.fori_loop(low, high, lambda t, c: (body(t), c)[1], 0)

    def everyone(body):
        for t in range(n_dp):
            o = wrap(dp + t, n_dp)
            each(1 if t == 0 else 0, n, lambda i: body(o, wrap(f + i, n)))

    barrier = pltpu.get_barrier_semaphore()

    def flip(index, bit):
        return index + bit * (1 - 2 * ((index // bit) % 2))

    peers = [(flip(dp, 1 << i), f) for i in range((n_dp - 1).bit_length())]
    peers += [(dp, flip(f, 1 << i)) for i in range((n - 1).bit_length())]

    def greet(o, g):
        pl.semaphore_signal(barrier, inc=1, device_id=(o, g), device_id_type=MESH)

    for o, g in peers:
        greet(o, g)

    @pl.when(a < depth - 1)
    def _():
        greet(dp, f + 2)

    @pl.when(a > 0)
    def _():
        greet(dp, f - 2)

    inner = jnp.where((a > 0) & (a < depth - 1), 1, 0)
    pl.semaphore_wait(barrier, len(peers) + 1 + inner)

    def greet_all():
        for i, (o, g) in enumerate(peers):
            pl.semaphore_signal(round_sem.at[i], inc=1, device_id=(o, g), device_id_type=MESH)
            pl.semaphore_wait(round_sem.at[i], 1)

    step = slab // chunks

    def piece(pa, pb, offset, rows, send_sem, recv_sem, device):
        part = wk.at[pa * 2 + pb, pl.ds(pl.multiple_of(offset, rows), rows), :]
        return pltpu.make_async_remote_copy(
            src_ref=part, dst_ref=part, send_sem=send_sem, recv_sem=recv_sem,
            device_id=device, device_id_type=MESH,
        )

    def half_at(k, c):
        return k * step + c * (step // 2)

    def quarter_at(k, c, x):
        return half_at(k, c) + x * (step // 4)

    half, quarter = step // 2, step // 4

    def up(pa, k):
        return piece(pa, b, half_at(k, core), half, zu_s.at[pa, k], z_r.at[pa, k], (dp, lax.rem(f + 2, n)))

    def down(pa, k):
        return piece(pa, b, half_at(k, core), half, zd_s.at[pa, k], z_r.at[pa, k], (dp, lax.rem(f + n - 2, n)))

    def cross_y(pa, pb, k):
        return piece(pa, pb, quarter_at(k, core, x_bit), quarter, y_s.at[pa, k], y_r.at[pa, k], (dp, 2 * a + 1 - b))

    def cross_x(pa, k, x):
        return piece(pa, 1 - b, quarter_at(k, core, x), quarter, x_s.at[pa, k], x_r.at[pa, k], (x_peer, f))

    def core_z(pa, k, c):
        return piece(pa, b, half_at(k, c), half, dz_s.at[pa, k], dz_r.at[pa, k], (partner, f))

    def core_y(pa, k, c):
        return piece(pa, 1 - b, quarter_at(k, c, x_bit), quarter, dy_s.at[pa, k], dy_r.at[pa, k], (partner, f))

    def core_x(pa, k, c):
        return piece(pa, 1 - b, quarter_at(k, c, 1 - x_bit), quarter, dx_s.at[pa, k], dx_r.at[pa, k], (partner, f))

    loads[0].wait()
    for k in range(chunks):
        @pl.when(a < depth - 1)
        def _():
            up(a, k).start()

        @pl.when(a > 0)
        def _():
            down(a, k).start()

        cross_y(a, b, k).start()

    def give(slot, send, recv, g):
        pltpu.make_async_remote_copy(
            src_ref=send.at[g], dst_ref=recv.at[f], send_sem=a2a_send.at[slot],
            recv_sem=a2a_recv.at[slot], device_id=(dp, g), device_id_type=MESH,
        ).start()

    def exchange(slot, send, recv):
        each(1, n, lambda t: give(slot, send, recv, wrap(f + t, n)))
        recv[f] = send[f]

    def arrived(slot, recv, count):
        blocks = recv.at[pl.ds(0, count)]
        pltpu.make_async_copy(blocks, blocks, a2a_recv.at[slot]).wait()

    def sent(slot, recv, count):
        blocks = recv.at[pl.ds(0, count)]
        pltpu.make_async_copy(blocks, blocks, a2a_send.at[slot]).wait()

    loads[1].wait()
    loads[2].wait()
    last = lengths[0] - 1
    picks = lax.broadcasted_iota(jnp.int32, (16, seq_len), 1) == last
    picks = jnp.where(picks, 1.0, 0.0).astype(BF16)
    row = jnp.concatenate(
        [
            jnp.dot(picks, hid[:, g * slab:(g + 1) * slab], preferred_element_type=F32)[:1]
            for g in range(n)
        ],
        axis=1,
    )
    scale = lax.rsqrt(jnp.mean(row * row, axis=-1, keepdims=True) + 1e-05)
    row_normed = (row * scale * again[...]).astype(BF16).astype(F32)
    for g in range(n):
        x_send[g] = row_normed[:, g * slab:(g + 1) * slab]
        last_in[g:g + 1, :] = row[:, g * slab:(g + 1) * slab]
    greet_all()
    exchange(0, x_send, x_recv)

    block = 16

    def normalise(i, carry):
        window = pl.ds(pl.multiple_of(i * block, block), block)
        x = hid[window, :].astype(F32)
        r = lax.rsqrt(jnp.mean(x * x, axis=-1, keepdims=True) + 1e-05)
        normed[window, :] = (x * r * again[...]).astype(BF16)
        return carry

    lax.fori_loop(0, seq_len // block, normalise, 0)

    def partial_queries():
        loads[3].wait()
        arrived(0, x_recv, n - 1)
        x_all = jnp.concatenate([x_recv[i] for i in range(n)], axis=0).astype(BF16)
        for h in range(HEADS):
            q_send[:, h, :] = jnp.dot(
                x_all, wq[:, h * HEAD:(h + 1) * HEAD], preferred_element_type=F32
            )
        exchange(1, q_send, q_recv)

    acc[...] = jnp.zeros_like(acc)

    def accumulate(slab_index):
        columns = pl.ds(pl.multiple_of(slab_index * slab, slab), slab)
        acc[...] += jnp.dot(normed[:, columns], wk[slab_index], preferred_element_type=F32)

    accumulate(f)

    def around(e, body):
        for sign in (1, -1):
            pa = a + sign * e
            valid = (pa >= 0) & (pa < depth) & (e >= (0 if sign == 1 else 1))

            @pl.when(valid)
            def _():
                body(pa, sign)

    def gather_step(d, carry):
        def from_z(pa, sign):
            for k in range(chunks):
                up(pa, k).wait_recv()
                if sign == 1:
                    @pl.when(a > 0)
                    def _():
                        down(pa, k).start()
                else:
                    @pl.when(a < depth - 1)
                    def _():
                        up(pa, k).start()
                cross_y(pa, b, k).start()
                core_z(pa, k, core).start()

        def from_y(pa, sign):
            for k in range(chunks):
                cross_y(pa, 1 - b, k).wait_recv()
                cross_x(pa, k, x_bit).start()
                core_y(pa, k, core).start()

        def from_x(pa, sign):
            for k in range(chunks):
                cross_x(pa, k, 1 - x_bit).wait_recv()
                core_x(pa, k, core).start()

        def consume(pa, sign):
            @pl.when(pa != a)
            def _():
                for k in range(chunks):
                    core_z(pa, k, 1 - core).wait_recv()
                accumulate(pa * 2 + b)

            for k in range(chunks):
                core_y(pa, k, 1 - core).wait_recv()
                core_x(pa, k, 1 - core).wait_recv()
            accumulate(pa * 2 + 1 - b)

        @pl.when(d >= 1)
        def _():
            around(d, from_z)
            around(d - 1, from_y)

        @pl.when(d >= 2)
        def _():
            around(d - 2, from_x)

        @pl.when(d == 2)
        def _():
            partial_queries()

        @pl.when(d >= 3)
        def _():
            around(d - 3, consume)

        return carry

    lax.fori_loop(1, depth + 3, gather_step, 0)

    for load in loads[4:]:
        load.wait()
    arrived(1, q_recv, n - 1)
    queries = jnp.sum(q_recv[...], axis=0)
    at_last = lax.broadcasted_iota(jnp.int32, cos_t.shape, 0) == last
    q_cos = jnp.sum(jnp.where(at_last, cos_t[...], 0.0), axis=0, keepdims=True)
    q_sin = jnp.sum(jnp.where(at_last, sin_t[...], 0.0), axis=0, keepdims=True)
    queries = queries * q_cos + pltpu.roll(queries, HEAD // 2, 1) * q_sin
    queries = (queries * (1.0 / math.sqrt(HEAD))).astype(BF16)

    scores = jnp.zeros((HEADS, seq_len), F32)
    head_of = lax.broadcasted_iota(jnp.int32, scores.shape, 0) // GROUP
    for kv in range(KV_HEADS):
        keys = acc[:, kv * HEAD:(kv + 1) * HEAD]
        keys = (keys * cos_t[...] + pltpu.roll(keys, HEAD // 2, 1) * sin_t[...]).astype(BF16)
        part = lax.dot_general(queries, keys, (((1,), (1,)), ((), ())), preferred_element_type=F32)
        scores = jnp.where(head_of == kv, part, scores)
    visible = lax.broadcasted_iota(jnp.int32, scores.shape, 1) < lengths[0]
    scores = jnp.where(visible, scores, -jnp.inf)
    powers = jnp.exp(scores - jnp.max(scores, axis=-1, keepdims=True))
    weights = (powers / jnp.sum(powers, axis=-1, keepdims=True)).astype(BF16)

    def weighted(g):
        columns = pl.ds(pl.multiple_of(g * slab, slab), slab)
        return jnp.dot(weights, normed[:, columns], preferred_element_type=F32)

    for t in range(1, n):
        g = wrap(f + t, n)
        u_send[g] = weighted(g)
        give(2, u_send, u_recv, g)
    u_recv[f] = weighted(f)
    arrived(2, u_recv, n - 1)
    sums = u_recv[...].reshape(n * HEADS, slab)
    top = sums.astype(BF16)
    rest = sums - top.astype(F32)
    middle = rest.astype(BF16)
    low = (rest - middle.astype(F32)).astype(BF16)
    values = wv[...]
    product = (
        jnp.dot(low, values, preferred_element_type=F32)
        + jnp.dot(middle, values, preferred_element_type=F32)
    ) + jnp.dot(top, values, preferred_element_type=F32)
    for kv in range(KV_HEADS):
        mixed[kv] = product[:, kv * HEAD:(kv + 1) * HEAD]

    share = HEADS * HEAD // n
    for h in range(HEADS):
        kv = h // GROUP
        part = mixed[kv, pl.ds(h, n, stride=HEADS), :]
        if share >= HEAD:
            at = h * HEAD % share
            c_send[h * HEAD // share, :, at:at + HEAD] = part
        else:
            pieces = HEAD // share
            for i in range(pieces):
                c_send[h * pieces + i] = part[:, i * share:(i + 1) * share]
    exchange(3, c_send, c_recv)
    arrived(3, c_recv, n - 1)
    context = jnp.sum(c_recv[...], axis=0).astype(BF16)
    for g in range(n):
        o_send[:, g, :] = jnp.dot(
            context, wo[:, g * slab:(g + 1) * slab], preferred_element_type=F32
        )
        gain2[g:g + 1, :] = fgain[:, g * slab:(g + 1) * slab]
    exchange(4, o_send, o_recv)

    lists = lax.broadcasted_iota(jnp.int32, owners.shape, 1)

    def owner_of(r):
        held = jnp.where(lists == list_ids[r], owners[...], 0)
        return jnp.sum(held.astype(F32), axis=1, keepdims=True)

    owner = owner_of(f)

    def count(r, slot):
        same = jnp.where(owner_of(r) == owner, 1.0, 0.0)
        return slot + same * jnp.where(r < f, 1.0, 0.0)

    code = owner * cap + lax.fori_loop(0, n, count, jnp.zeros((1, 1), F32))

    arrived(4, o_recv, n - 1)
    scaled = (last_in[...] + jnp.sum(o_recv[...], axis=0)) * gain2[...]
    square = jnp.sum(jnp.sum(scaled * scaled, axis=1, keepdims=True), axis=0, keepdims=True)
    embedded = (scaled * lax.rsqrt(square / width + 1e-06)).astype(BF16).astype(F32)
    for g in range(n):
        e_send[g, :, :slab] = embedded[g:g + 1, :]
        e_send[g, :, slab:] = jnp.broadcast_to(code, (1, 128))

    def post(o, g):
        pltpu.make_async_remote_copy(
            src_ref=e_send.at[g], dst_ref=e_recv.at[me], send_sem=a2a_send.at[5],
            recv_sem=a2a_recv.at[5], device_id=(o, g), device_id_type=MESH,
        ).start()

    everyone(post)
    e_recv[me] = e_send[f]
    arrived(5, e_recv, total - 1)

    first = (dp * cap).astype(F32)
    for j in range(n_dp):
        rows = jnp.concatenate([e_recv[j * n + i] for i in range(n)], axis=0)
        codes = rows[:, slab:slab + 1]
        for s in range(cap):
            kept = jnp.where(codes == first + s, rows[:, :slab], 0.0)
            out_ref[0, j, s:s + 1, :] = jnp.sum(kept, axis=0, keepdims=True).astype(BF16)

    for index, recv in ((0, x_recv), (1, q_recv), (2, u_recv), (3, c_recv), (4, o_recv)):
        sent(index, recv, n - 1)
    sent(5, e_recv, total - 1)

    def drain(pa, carry):
        for k in range(chunks):
            @pl.when((pa <= a) & (a < depth - 1))
            def _():
                up(pa, k).wait_send()

            @pl.when((pa >= a) & (a > 0))
            def _():
                down(pa, k).wait_send()

            @pl.when(pa != a)
            def _():
                core_z(pa, k, core).wait_send()

            cross_y(pa, b, k).wait_send()
            cross_x(pa, k, x_bit).wait_send()
            core_y(pa, k, core).wait_send()
            core_x(pa, k, core).wait_send()
        return carry

    lax.fori_loop(0, depth, drain, 0)


def local(
    n_dp, n,
    hidden, lengths, list_ids, list_owner, attn_gain, final_gain, w_query, w_key, w_value, w_out,
):
    _, seq_len, width = hidden.shape
    slab = width // n
    depth = n // 2
    chunks = 2 if n <= 8 else 1
    cap = max(2, 2 * n // n_dp)
    share = HEADS * HEAD // n
    cosine, sine = rope_tables(seq_len)
    pieces = pltpu.SemaphoreType.DMA((depth, chunks))
    any_spec = pl.BlockSpec(memory_space=pl.ANY)
    smem_spec = pl.BlockSpec(memory_space=pltpu.SMEM)
    vmem = pltpu.VMEM
    return pl.pallas_call(
        functools.partial(kernel, n_dp, n, chunks),
        out_shape=jax.ShapeDtypeStruct((1, n_dp, cap, slab), BF16),
        in_specs=[smem_spec] * 2 + [any_spec] * 10,
        out_specs=pl.BlockSpec(memory_space=pltpu.VMEM),
        scratch_shapes=[
            vmem((seq_len, width), BF16),
            vmem((seq_len, width), BF16),
            vmem((1, width), F32),
            vmem((1, width), F32),
            vmem((seq_len, HEAD), F32),
            vmem((seq_len, HEAD), F32),
            vmem(w_query.shape, BF16),
            vmem((n,) + w_key.shape, BF16),
            vmem(w_value.shape, BF16),
            vmem(w_out.shape, BF16),
            vmem((1, list_owner.shape[0]), jnp.int32),
            vmem((seq_len, KV_HEADS * HEAD), F32),
            vmem((n, slab), F32),
            vmem((n, slab), F32),
            vmem((n, 1, slab), F32),
            vmem((n, 1, slab), F32),
            vmem((n, HEADS, HEAD), F32),
            vmem((n, HEADS, HEAD), F32),
            vmem((n, HEADS, slab), F32),
            vmem((n, HEADS, slab), F32),
            vmem((KV_HEADS, n * HEADS, HEAD), F32),
            vmem((n, n, share), F32),
            vmem((n, n, share), F32),
            vmem((n, n, slab), F32),
            vmem((n, n, slab), F32),
            vmem((n, 1, slab + 128), F32),
            vmem((n_dp * n, 1, slab + 128), F32),
            pltpu.SemaphoreType.DMA((10,)),
            pltpu.SemaphoreType.DMA((6,)),
            pltpu.SemaphoreType.DMA((6,)),
            pltpu.SemaphoreType.REGULAR(((n_dp - 1).bit_length() + (n - 1).bit_length(),)),
        ] + [pieces] * 13,
        compiler_params=pltpu.CompilerParams(
            collective_id=0, has_side_effects=True, vmem_limit_bytes=67043328
        ),
    )(
        lengths, list_ids,
        list_owner.reshape(1, -1), hidden, attn_gain.reshape(1, width), final_gain.reshape(1, width),
        cosine, sine, w_query, w_key, w_value, w_out,
    )


def solution(mesh):
    in_specs = (
        P(("dp", "fsdp"), None, None),
        P(("dp", "fsdp")),
        P("dp"),
        P(),
        P(),
        P(),
        P("fsdp", None),
        P("fsdp", None),
        P("fsdp", None),
        P("fsdp", None),
    )
    out_specs = P("dp", None, None, "fsdp")
    body = functools.partial(local, mesh.shape["dp"], mesh.shape["fsdp"])
    return jax.shard_map(body, mesh=mesh, in_specs=in_specs, out_specs=out_specs, check_vma=False)
```
